32 devices in a mesh: groups: 2 (over y), mp: 2 (over x), expert: 4 (over z), dp: 2 (over core).
Axes of the slice: x: 2, y: 2, z: 4, core: 2. Of those that a mesh axis runs over, the one named last changes fastest.
Arguments:
- hidden_in: bfloat16 [1024, 4096], P(('groups', 'expert', 'dp'), 'mp'), parts along dimension 0, may hold values from -6 to 6
- norm_gain: bfloat16 [2, 4096], P(None, 'mp'), may hold values from 0.25 to 1.75
- expert_ids: int32 [2, 1024, 2], P(None, ('groups', 'expert', 'dp')), parts along dimension 1, may hold values from 0 to 3, all different within a row; in each aligned block of 64 rows (0 to 63, 64 to 127, ..., all dimensions but the last counted through in order) at most 64 rows name the same one
- gate_counts: int32 [2, 1024, 2], P(None, ('groups', 'expert', 'dp')), parts along dimension 1, may hold values from 8 to 15
- exit_layer: int32 [1024], P(('groups', 'expert', 'dp')), parts along dimension 0, may hold values from 1 to 2
- w_gate: bfloat16 [2, 4, 7168, 4096], P(None, 'expert', ('mp', 'dp')), may hold values from -0.09375 to 0.09375
- w_up: bfloat16 [2, 4, 7168, 4096], P(None, 'expert', ('mp', 'dp')), may hold values from -0.09375 to 0.09375
- w_down: bfloat16 [2, 4, 7168, 4096], P(None, 'expert', ('mp', 'dp')), may hold values from -0.0625 to 0.0625
Outputs:
- hidden_out: bfloat16 [1024, 4096], P(('groups', 'expert', 'dp'), 'mp'), parts along dimension 0
The draws below stay inside these ranges and needn't reach their ends.
There are 2 independent parts, one for each index of `groups`. The reference program is written for one: setup_inputs(seed, part) draws one part's arguments, and reference() takes and returns one part's arrays. A program takes and returns all parts, laid end to end along the dimension named above; an argument that names none is the same for every part. Nothing has to cross between parts.
Inputs may be any that keep to these rules, and one draw needn't show every extreme that they name: `expert_ids`: A token's two ids in a layer differ. In the rows of one device in one layer (aligned blocks of 64 rows, layer by layer) some expert may be named by all 64 rows.
All inputs are finite; a program needn't handle non-finite values.
Results may differ from the reference program's by a relative error of at most 0.014.
Values may be sent and summed in bfloat16 or wider, within the bound.
A program may use at most 384 MiB of HBM per device.

```python
import math
import jax
import jax.numpy as jnp
import numpy as np
from jax import lax

D = 4096
FF = 7168
LAYERS = 2
TOK_DEV = 64
EXPERTS = 4
TOKENS = 512
N_MP = 2


def draw_exit_layer(key, part):
    own_key = jax.random.fold_in(key, 17)
    key_roll, key_early = jax.random.split(own_key)
    roll_value = jax.random.randint(key_roll, (TOKENS,), 0, 100)
    early_exit = jax.random.randint(key_early, (TOKENS,), 1, max(LAYERS, 2))
    exits = jnp.where(roll_value < 95, LAYERS, early_exit)
    position = jnp.arange(TOKENS)
    exits = jnp.where(position == 0, 1, jnp.where(position == 1, LAYERS, exits))
    return exits.astype(jnp.int32)


def place_ends(array, stream_key, least, largest):
    place = [jax.random.randint(jax.random.fold_in(stream_key, axis), (), 0, length) for axis, length in enumerate(array.shape)]
    main_axis = array.shape.index(max(array.shape))
    beside = place[:main_axis] + [(place[main_axis] + 1) % array.shape[main_axis]] + place[main_axis + 1:]
    return array.at[tuple(place)].set(least).at[tuple(beside)].set(largest)


def shard_levels(rng, dims, cuts, smallest, high):
    def one(dim, parts):
        steps = jax.random.uniform(jax.random.fold_in(jax.random.fold_in(rng, 6), dim), (parts,), jnp.float32, smallest / len(cuts), high / len(cuts))
        return jnp.repeat(jnp.exp(steps), dims[dim] // parts).reshape((-1,) + (1,) * (len(dims) - dim - 1))

    loudness = one(*cuts[0])
    for cut in cuts[1:]:
        loudness = loudness * one(*cut)
    return loudness


def routed_block(key, own, number, rows, amount, top, limit, skew):
    order = jax.random.permutation(key, amount)
    packed, ordinary = portions_of(amount, rows * top, limit, skew, True), portions_of(amount, rows * top, limit, skew, False)
    places = jnp.arange(amount)

    def named(sizes, turn):
        used = int((sizes > 0).sum())
        fixed = max(1, used // 4)
        shifted = fixed + (places - fixed + turn * (used - fixed)) % max(1, amount - fixed)
        return jnp.zeros((amount,), jnp.int32).at[order[jnp.where(places < fixed, places, shifted)]].set(jnp.asarray(sizes, jnp.int32))

    sizes = jnp.where(number % 4 == 0, named(packed, number // 4), named(ordinary, number - number // 4 - 1))
    mixed = jax.random.permutation(jax.random.fold_in(own, 3), amount)
    source_of, taker = mixed[0:amount // 2 * 2:2], mixed[1:amount // 2 * 2:2]
    slack = jnp.minimum(sizes[source_of] - 1, limit - sizes[taker]) // 2
    slack = jnp.where((source_of == order[0]) | (taker == order[0]) | (sizes[taker] == 0), 0, jnp.maximum(slack, 0))
    shifted = jax.random.randint(jax.random.fold_in(own, 4), (amount // 2,), 0, 1 << 20) % (slack + 1)
    sizes = sizes.at[source_of].add(-shifted).at[taker].add(shifted)
    members = jnp.searchsorted(jnp.cumsum(sizes), jnp.arange(rows * top), side="right").astype(jnp.int32)
    table = members.reshape(top, rows).T
    table = table[jax.random.permutation(jax.random.fold_in(own, 1), rows)]
    turn = jax.random.randint(jax.random.fold_in(own, 2), (rows, 1), 0, top)
    return jnp.take_along_axis(table, (jnp.arange(top)[None, :] + turn) % top, axis=1)


def portions_of(count, total, reach, lean, full):
    portions = [(1 << 20) // math.isqrt(standing ** lean) + 1 for standing in range(1, count + 1)]
    largest = reach if full else min(reach, max(-(-total // count), total * portions[0] // sum(portions)))
    least = 1 if total - largest >= count - 1 else 0
    holding, surplus = [largest] + [least] * (count - 1), total - largest - least * (count - 1)
    while surplus > 0:
        free = [i for i in range(1, count) if holding[i] < largest] or [i for i in range(1, count) if holding[i] < reach]
        whole, left = sum([portions[i] for i in free]), surplus
        for i in free:
            more = min(reach - holding[i], max(1, left * portions[i] // whole), surplus)
            holding[i] = holding[i] + more
            surplus = surplus - more
    return np.array(holding)


def centred(key, shape, deviation, most, pieces=(), held_as=jnp.bfloat16):
    drawn = jax.random.normal(key, shape, jnp.float32) * deviation
    if len(pieces) > 0:
        drawn = shard_levels(key, shape, pieces, -0.22, 0.18) * drawn
    return jnp.clip(drawn, min=-most, max=most).astype(held_as)


def setup_inputs(seed: int = 0, part: int = 0) -> dict:
    key_of = jax.random.split(jax.random.key(seed), 9)
    own_keys = jax.random.split(jax.random.fold_in(key_of[8], part), 9)
    hidden_in = centred(own_keys[0], (TOKENS, D), 1.0, 6.0, ((0, 8), (1, 2)))
    norm_gain = jnp.clip(1.0 + 0.15 * jax.random.normal(key_of[1], (LAYERS, D), jnp.float32), 0.25, 1.75).astype(jnp.bfloat16)
    expert_ids_keys = jax.random.split(jax.random.fold_in(own_keys[2], 1), LAYERS * TOKENS // TOK_DEV)
    expert_ids_turns = jax.random.permutation(jax.random.fold_in(own_keys[2], 3), LAYERS * TOKENS // TOK_DEV)
    expert_ids = jax.vmap(lambda own, number: routed_block(jax.random.fold_in(own_keys[2], 2), own, number, TOK_DEV, EXPERTS, 2, TOK_DEV, 2))(expert_ids_keys, expert_ids_turns).reshape((LAYERS, TOKENS, 2))
    gate_counts = place_ends(jax.random.randint(own_keys[3], (LAYERS, TOKENS, 2), 8, 16), jax.random.fold_in(own_keys[3], 1), 8, 15).astype(jnp.int32)
    exit_layer = draw_exit_layer(jax.random.fold_in(jax.random.fold_in(key_of[8], part), 71), part)
    w_gate = centred(key_of[5], (LAYERS, EXPERTS, FF, D), D ** -0.5, 0.09375, ((1, 4), (2, 4)))
    w_up = centred(key_of[6], (LAYERS, EXPERTS, FF, D), D ** -0.5, 0.09375, ((1, 4), (2, 4)))
    w_down = centred(key_of[7], (LAYERS, EXPERTS, FF, D), FF ** -0.5, 0.0625, ((1, 4), (2, 4)))
    return {"hidden_in": hidden_in, "norm_gain": norm_gain, "expert_ids": expert_ids, "gate_counts": gate_counts, "exit_layer": exit_layer, "w_gate": w_gate, "w_up": w_up, "w_down": w_down}


norm_floor = 0.1

def expert_output(normed, gate_rows, up_rows, down_rows):
    contract = (((1,), (1,)), ((), ()))
    gate_val = lax.dot_general(normed, gate_rows, contract, preferred_element_type=jnp.float32)
    up_val = lax.dot_general(normed, up_rows, contract, preferred_element_type=jnp.float32)
    hidden = (jax.nn.silu(gate_val) * up_val).astype(jnp.bfloat16)
    block_len = FF // N_MP
    running = jnp.zeros((normed.shape[0], D), jnp.float32)
    for block_idx in range(N_MP):
        row_start = block_idx * block_len
        partial_value = jnp.dot(hidden[:, row_start:row_start + block_len], down_rows[row_start:row_start + block_len], preferred_element_type=jnp.float32)
        rounded = lax.optimization_barrier(partial_value.astype(jnp.bfloat16))
        running = running + rounded.astype(jnp.float32)
    return running.astype(jnp.bfloat16)

def reference(hidden_in, norm_gain, expert_ids, gate_counts, exit_layer, w_gate, w_up, w_down):
    current = hidden_in
    expert_range = jnp.arange(EXPERTS, dtype=jnp.int32)
    for layer_idx in range(LAYERS):
        current_f32 = current.astype(jnp.float32)
        sum_squares = lax.optimization_barrier(jnp.sum(current_f32 * current_f32, axis=1, keepdims=True))
        inv_rms = lax.rsqrt(sum_squares / D + norm_floor)
        normed = (current_f32 * inv_rms * norm_gain[layer_idx].astype(jnp.float32)[None, :]).astype(jnp.bfloat16)
        outputs = lax.map(lambda weights: expert_output(normed, weights[0], weights[1], weights[2]), (w_gate[layer_idx], w_up[layer_idx], w_down[layer_idx]))
        counts = gate_counts[layer_idx].astype(jnp.float32)
        gate_share = counts / lax.optimization_barrier(jnp.sum(counts, axis=1, keepdims=True))
        matched = expert_ids[layer_idx][:, :, None] == expert_range[None, None, :]
        weight_te = lax.optimization_barrier(jnp.sum(jnp.where(matched, gate_share[:, :, None], jnp.float32(0.0)), axis=1))
        active = (exit_layer > layer_idx).astype(jnp.float32)
        weight_te = weight_te * active[:, None]
        update = jnp.einsum('te,etd->td', weight_te, outputs.astype(jnp.float32), precision=lax.Precision.HIGHEST)
        current = (current_f32 + update).astype(jnp.bfloat16)
    return current
```

```python
import functools

import jax
import jax.numpy as jnp
from jax import lax
from jax.experimental import pallas as pl
from jax.experimental.pallas import tpu as pltpu
from jax.sharding import PartitionSpec as P

LAYERS = 2
HALVES = 2
PARTS = 2
LANES = 128

norm_floor = 0.1
MESH = pl.DeviceIdType.MESH
CHUNK = 16


def tile_of(length, best):
    tile = best
    while tile >= 128:
        if length % tile == 0:
            return tile
        tile //= 2
    return length


def stack_kernel(
    n, dp, mp,
    cur_ref, gain_ref, share_ref, wg_hbm, wu_hbm, wd_hbm, out_ref,
    wg, wu, wd, xg, p, rd, xr, rzu, rzd, hid, col, inv, shares,
    w_sem, sh_s, sh_r, zu_s, zu_r, zd_s, zd_r, x_s, x_r, d_s, d_r,
    sw_s, sw_r, bx_s, bx_r, bu_s, bu_r, bd_s, bd_r,
):
    rows, width = cur_ref.shape
    full = width * mp
    units = wg.shape[0]
    hr = rows // HALVES
    pr = hr // PARTS
    core_rows = n * hr
    size = dp * core_rows
    e, m, d = lax.axis_index("expert"), lax.axis_index("mp"), lax.axis_index("dp")
    tile = tile_of(units, 256)
    steps = units // tile
    ctile = tile_of(width, 1024)
    csteps = width // ctile
    contract = (((1,), (1,)), ((), ()))

    def part(r):
        return lax.rem(m - r + mp, mp)

    def ahead(r):
        return {"mp": lax.rem(m + r, mp)}

    def core(k):
        return lax.rem(d + k, dp)

    place_of = {k: e + k for k in range(1 - n, n)}
    has = {k: (e + k <= n - 1 if k > 0 else e + k >= 0) for k in range(1 - n, n) if k}
    below, above = e > 0, e < n - 1
    up_z, down_z = {"expert": lax.rem(e + 1, n)}, {"expert": lax.rem(e + n - 1, n)}

    def remote(src, dst, ss, rs, dev):
        return pltpu.make_async_remote_copy(
            src_ref=src, dst_ref=dst, send_sem=ss, recv_sem=rs, device_id=dev, device_id_type=MESH
        )

    def when(cond, run):
        if cond is None:
            run()
        else:
            pl.when(cond)(run)

    sent = {}

    def send(group, make, *conds):
        make().start()
        sent.setdefault(group, []).append((make, conds))

    def drain(group):
        for make, conds in sent.pop(group, []):
            cond = None
            for c in conds:
                cond = c if cond is None else jnp.logical_and(cond, c)
            when(cond, lambda make=make: make().wait_send())

    def weight(layer_idx, i):
        src, dst = ((wg_hbm, wg), (wu_hbm, wu), (wd_hbm, wd))[i]
        return pltpu.make_async_copy(src.at[layer_idx, 0], dst, w_sem.at[i])

    def row_of(c, blk, j=0):
        return pl.multiple_of((c * n + blk) * hr + j * pr, pr)

    def block_ref(h, blk, j, c, q):
        return xg.at[h, q, pl.ds(row_of(c, blk, j), pr)]

    def zu(h, s, j, blk):
        ref = block_ref(h, blk, j, d, m)
        return remote(ref, ref, zu_s.at[h, s, j], zu_r.at[h, s, j], up_z)

    def zd(h, s, j, blk):
        ref = block_ref(h, blk, j, d, m)
        return remote(ref, ref, zd_s.at[h, s, j], zd_r.at[h, s, j], down_z)

    def xm(h, blk, j, r, q):
        ref = block_ref(h, blk, j, d, q)
        return remote(ref, ref, x_s.at[h, blk, j, r], x_r.at[h, blk, j, r], ahead(r))

    def dc(h, blk, j, r, k, c):
        ref = block_ref(h, blk, j, c, part(r))
        return remote(ref, ref, d_s.at[h, blk, j, r, k], d_r.at[h, blk, j, r, k], {"dp": core(k)})

    def spread(h, j, blk, *conds):
        for r in range(1, mp):
            send(("gather", h), lambda r=r: xm(h, blk, j, r, m), *conds)
        to_core(h, blk, j, 0, *conds)

    def to_core(h, blk, j, r, *conds):
        for k in range(1, dp):
            send(("gather", h), lambda k=k: dc(h, blk, j, r, k, d), *conds)

    def own_z(h, j):
        pl.when(above)(lambda: send(("gather", h), lambda: zu(h, 1, j, e), above))
        pl.when(below)(lambda: send(("gather", h), lambda: zd(h, 1, j, e), below))

    def z_step(h, s, j):
        low, high = place_of[-s], place_of[s]

        def from_below():
            zu(h, s, j, low).wait_recv()
            if s + 1 < n:
                pl.when(above)(
                    lambda: send(("gather", h), lambda: zu(h, s + 1, j, low), has[-s], above)
                )
            spread(h, j, low, has[-s])

        def from_above():
            zd(h, s, j, high).wait_recv()
            if s + 1 < n:
                pl.when(below)(
                    lambda: send(("gather", h), lambda: zd(h, s + 1, j, high), has[s], below)
                )
            spread(h, j, high, has[s])

        pl.when(has[-s])(from_below)
        pl.when(has[s])(from_above)

    def x_step(h, s):
        def take(blk, *conds):
            for j in range(PARTS):
                for r in range(1, mp):
                    xm(h, blk, j, r, part(r)).wait_recv()
                    to_core(h, blk, j, r, *conds)

        if s == 0:
            take(e)
        else:
            pl.when(has[-s])(lambda: take(place_of[-s], has[-s]))
            pl.when(has[s])(lambda: take(place_of[s], has[s]))

    def core_done(h):
        for k in range(1, dp):
            for blk in range(n):
                for j in range(PARTS):
                    for r in range(mp):
                        dc(h, blk, j, r, k, core(dp - k)).wait_recv()

    def own_rows(h, layer_idx, current):
        gain = gain_ref[...].astype(jnp.float32)[layer_idx:layer_idx + 1, :]
        lanes = lax.broadcasted_iota(jnp.int32, (CHUNK, LANES), 1)

        def chunk(i, _):
            at = pl.ds(pl.multiple_of(h * hr + i * CHUNK, CHUNK), CHUNK)
            v = current[at, :].astype(jnp.float32)
            left = jnp.sum(v * v, axis=1, keepdims=True)
            tail = jnp.zeros((CHUNK, LANES), jnp.float32)
            for lane in range(3):
                held = left.astype(jnp.bfloat16).astype(jnp.float32)
                tail = jnp.where(lanes == lane, held, tail)
                left = left - held
            to = pl.ds(pl.multiple_of(row_of(d, e) + i * CHUNK, CHUNK), CHUNK)
            xg[h, m, to, 0:width] = (v * gain).astype(jnp.bfloat16)
            xg[h, m, to, width:width + LANES] = tail.astype(jnp.bfloat16)
            return 0

        lax.fori_loop(0, hr // CHUNK, chunk, 0)

    def scales(h, layer_idx):
        total = jnp.zeros((size, 1), jnp.float32)
        for q in range(mp):
            tail = xg[h, q, :, width:width + LANES].astype(jnp.float32)
            total = total + jnp.sum(tail, axis=1, keepdims=True)
        scale = lax.rsqrt(total / full + norm_floor)
        inv[0] = scale
        inv[1] = scale * col[layer_idx, h]

    def hidden(h, layer_idx, events):
        def step(t, _):
            at = pl.ds(pl.multiple_of(t * tile, tile), tile)
            g = u = None
            for q in range(mp):
                a = xg[h, q, :, 0:width]
                wide = slice(q * width, (q + 1) * width)
                gq = lax.dot_general(a, wg[at, wide], contract, preferred_element_type=jnp.float32)
                uq = lax.dot_general(a, wu[at, wide], contract, preferred_element_type=jnp.float32)
                g, u = (gq, uq) if q == 0 else (g + gq, u + uq)
            g = g * inv[0]
            y = g / (1.0 + jnp.exp(-g)) * (u * inv[1])
            hid[:, at] = y.astype(jnp.bfloat16)
            for place, run in events:
                if steps == 1:
                    run()
                else:
                    pl.when(t == min(place * steps // 7, steps - 1))(run)
            return 0

        if steps == 1:
            step(0, 0)
        else:
            lax.fori_loop(0, steps, step, 0)

    def project(h, first, count):
        def step(t, _):
            q = part(first + t // csteps)
            off = lax.rem(t, csteps) * ctile
            wide = pl.ds(pl.multiple_of(q * width + off, ctile), ctile)
            y = jnp.dot(hid[...], wd[:, wide], preferred_element_type=jnp.float32)
            p[h, q, :, pl.ds(pl.multiple_of(off, ctile), ctile)] = y.astype(jnp.bfloat16)
            return 0

        lax.fori_loop(0, count * csteps, step, 0)

    def swap(h, q, r, k):
        src = p.at[h, q, pl.ds(pl.multiple_of(core(k) * core_rows, core_rows), core_rows)]
        return remote(src, rd.at[h, k - 1, q], sw_s.at[h, r, k], sw_r.at[h, r, k], {"dp": core(k)})

    def swap_start(h, r):
        for k in range(1, dp):
            send(("home", h), lambda k=k: swap(h, part(r), r, k))

    def swap_wait(h, r):
        for k in range(1, dp):
            swap(h, part(r), r, k).wait_recv()

    def chunks(j, count, run):
        def chunk(i, _):
            run(pl.multiple_of(j * pr + i * CHUNK, CHUNK))
            return 0

        if count == CHUNK:
            chunk(0, 0)
        else:
            lax.fori_loop(0, count // CHUNK, chunk, 0)

    def with_cores(h, q, blk, off):
        at = pl.ds(pl.multiple_of(row_of(d, blk) + off, CHUNK), CHUNK)
        other = pl.ds(pl.multiple_of(blk * hr + off, CHUNK), CHUNK)
        v = p[h, q, at, :].astype(jnp.float32)
        for k in range(1, dp):
            v = v + rd[h, k - 1, q, other, :].astype(jnp.float32)
        return at, other, v

    def bx(h, blk, j, r):
        src = p.at[h, part(r), pl.ds(row_of(d, blk, j), pr)]
        dst = xr.at[h, r - 1, pl.ds(pl.multiple_of(blk * hr + j * pr, pr), pr)]
        return remote(src, dst, bx_s.at[h, blk, j, r], bx_r.at[h, blk, j, r], {"mp": part(r)})

    def by_distance(k, run):
        if k == 0:
            run(e)
        else:
            pl.when(has[k])(lambda: run(place_of[k], has[k]))
            pl.when(has[-k])(lambda: run(place_of[-k], has[-k]))

    def back_x(h, k):
        def run(blk, *conds):
            for j in range(PARTS):
                for r in range(1, mp):
                    def put(off, q=part(r)):
                        at, _, v = with_cores(h, q, blk, off)
                        p[h, q, at, :] = v.astype(jnp.bfloat16)

                    chunks(j, pr, put)
                    send(("home", h), lambda j=j, r=r: bx(h, blk, j, r), *conds)

        by_distance(k, run)

    def bu(h, blk, j):
        src = p.at[h, m, pl.ds(row_of(d, blk, j), pr)]
        return remote(src, rzu.at[h, blk, pl.ds(j * pr, pr)], bu_s.at[h, blk, j], bu_r.at[h, blk, j], up_z)

    def bd(h, blk, j):
        src = p.at[h, m, pl.ds(row_of(d, blk, j), pr)]
        return remote(src, rzd.at[h, blk, pl.ds(j * pr, pr)], bd_s.at[h, blk, j], bd_r.at[h, blk, j], down_z)

    def gathered(h, blk, off):
        at, other, v = with_cores(h, m, blk, off)
        for r in range(1, mp):
            v = v + xr[h, r - 1, other, :].astype(jnp.float32)
        return at, v

    def plain(h, blk, j):
        def put(off):
            at, v = gathered(h, blk, off)
            p[h, m, at, :] = v.astype(jnp.bfloat16)

        chunks(j, pr, put)

    def joined(h, blk, j, incoming):
        def put(off):
            at, v = gathered(h, blk, off)
            v = v + incoming[h, blk, pl.ds(off, CHUNK), :].astype(jnp.float32)
            p[h, m, at, :] = v.astype(jnp.bfloat16)

        chunks(j, pr, put)

    def back_z(h, k, j):
        def along(blk, cond, copy, inner, incoming):
            for r in range(1, mp):
                bx(h, blk, j, r).wait_recv()

            @pl.when(inner)
            def _():
                copy(h, blk, j).wait_recv()
                joined(h, blk, j, incoming)

            pl.when(jnp.logical_not(inner))(lambda: plain(h, blk, j))
            send(("home", h), lambda: copy(h, blk, j), cond)

        pl.when(has[k])(lambda: along(place_of[k], has[k], bu, below, rzu))
        pl.when(has[-k])(lambda: along(place_of[-k], has[-k], bd, above, rzd))

    def arrive(h, current):
        for j in range(PARTS):
            for r in range(1, mp):
                bx(h, e, j, r).wait_recv()
            pl.when(below)(lambda j=j: bu(h, e, j).wait_recv())
            pl.when(above)(lambda j=j: bd(h, e, j).wait_recv())

        def finish(sources):
            def put(off):
                _, v = gathered(h, e, off)
                for ref in sources:
                    v = v + ref[h, e, pl.ds(off, CHUNK), :].astype(jnp.float32)
                at = pl.ds(pl.multiple_of(h * hr + off, CHUNK), CHUNK)
                out_ref[at, :] = (current[at, :].astype(jnp.float32) + v).astype(jnp.bfloat16)

            chunks(0, hr, put)

        if n == 1:
            finish([])
        else:
            pl.when(jnp.logical_not(below))(lambda: finish([rzd]))
            pl.when(jnp.logical_not(above))(lambda: finish([rzu]))
            if n > 2:
                pl.when(jnp.logical_and(below, above))(lambda: finish([rzu, rzd]))

    slot = d * n + e
    shares[slot] = share_ref[...]
    own_rows(0, 0, cur_ref)
    barrier = pltpu.get_barrier_semaphore()
    others = [(k, c) for k in range(n) for c in range(dp) if k + c > 0]
    peers = [ahead(r) for r in range(1, mp)]
    peers += [{"expert": lax.rem(e + k, n), "dp": core(c)} for k, c in others]
    for dev in peers:
        pl.semaphore_signal(barrier, inc=1, device_id=dev, device_id_type=MESH)
    pl.semaphore_wait(barrier, len(peers))

    def share_copy(k, c, place):
        ref = shares.at[place]
        return remote(ref, ref, sh_s.at[k, c], sh_r.at[k, c],
                      {"expert": lax.rem(e + k, n), "dp": core(c)})

    def columns():
        for k, c in others:
            place = lax.rem(d - c + dp, dp) * n + lax.rem(e - k + n, n)
            share_copy(k, c, place).wait_recv()
        lanes = lax.broadcasted_iota(jnp.int32, (shares.shape[2], shares.shape[1]), 1)
        for place in range(n * dp):
            tokens = shares[place].T
            for layer_idx in range(LAYERS):
                picked = jnp.sum(
                    jnp.where(lanes == layer_idx * n + e, tokens, 0.0), axis=1, keepdims=True
                )
                for h in range(HALVES):
                    col[layer_idx, h, place * hr:(place + 1) * hr, :] = picked[h * hr:(h + 1) * hr]

    both = range(PARTS)
    far = list(range(n - 1, 0, -1))

    def start_own(h):
        for j in both:
            own_z(h, j)
            spread(h, j, e)

    def z_all(h, s):
        for j in both:
            z_step(h, s, j)

    def back_all(h, k):
        for j in both:
            back_z(h, k, j)

    for layer_idx in range(LAYERS):
        if layer_idx == 0:
            start_own(0)
            for k, c in others:
                send(("share", 0), lambda k=k, c=c: share_copy(k, c, slot))
            for i in range(3):
                weight(0, i).start()
            own_rows(1, 0, cur_ref)
            columns()
            for s in range(1, n):
                z_all(0, s)
                if s == n - 2:
                    start_own(1)
            if n < 3:
                start_own(1)
        else:
            arrive(0, cur_ref)
            own_rows(0, layer_idx, out_ref)
            start_own(0)
            for k in far:
                back_all(1, k)
                z_all(0, n - k)
            arrive(1, cur_ref)
            own_rows(1, layer_idx, out_ref)
            start_own(1)
        for s in range(n - 1):
            x_step(0, s)
        if n > 1:
            z_all(1, 1)
        x_step(0, n - 1)
        core_done(0)
        scales(0, layer_idx)
        weight(layer_idx, 0).wait()
        weight(layer_idx, 1).wait()
        events = [(2 * s - 4, lambda s=s: z_all(1, s)) for s in range(2, n)]
        events += [(2 + s, lambda s=s: x_step(1, s)) for s in range(n - 1)]
        hidden(0, layer_idx, events)
        weight(layer_idx, 2).wait()
        drain(("home", 0))
        drain(("gather", 0))
        project(0, 1, mp - 1)
        for r in range(1, mp):
            swap_start(0, r)
        x_step(1, n - 1)
        project(0, 0, 1)
        swap_start(0, 0)
        for r in range(1, mp):
            swap_wait(0, r)
        for k in far + [0]:
            back_x(0, k)
        swap_wait(0, 0)
        core_done(1)
        scales(1, layer_idx)
        rest = [(k, j) for k in far for j in both]
        late = rest[-1:]
        spots = [1, 2, 4, 5, 6]
        events = [
            (spots[min(i, 4)], lambda k=k, j=j: back_z(0, k, j)) for i, (k, j) in enumerate(rest[:-1])
        ]
        hidden(1, layer_idx, events)
        if layer_idx + 1 < LAYERS:
            weight(layer_idx + 1, 0).start()
            weight(layer_idx + 1, 1).start()
        drain(("home", 1))
        drain(("gather", 1))
        project(1, 1, mp - 1)
        for r in range(1, mp):
            swap_start(1, r)
        for k, j in late:
            back_z(0, k, j)
        project(1, 0, 1)
        swap_start(1, 0)
        if layer_idx + 1 < LAYERS:
            weight(layer_idx + 1, 2).start()
        for r in range(1, mp):
            swap_wait(1, r)
        for k in far + [0]:
            back_x(1, k)
        swap_wait(1, 0)
    arrive(0, out_ref)
    for k in far:
        back_all(1, k)
    arrive(1, out_ref)
    for group in list(sent):
        drain(group)


def stack(n, dp, mp, current, gain, share, w_gate, w_up, w_down):
    rows, width = current.shape
    units, full = w_gate.shape[2:]
    hr = rows // HALVES
    size = n * dp * hr
    bf, f32, dma = jnp.bfloat16, jnp.float32, pltpu.SemaphoreType.DMA
    vmem = pl.BlockSpec(memory_space=pltpu.VMEM)
    hbm = pl.BlockSpec(memory_space=pl.ANY)

    def pair(*shape):
        return [dma(shape), dma(shape)]

    return pl.pallas_call(
        functools.partial(stack_kernel, n, dp, mp),
        out_shape=jax.ShapeDtypeStruct((rows, width), bf),
        in_specs=[vmem, vmem, vmem, hbm, hbm, hbm],
        out_specs=vmem,
        scratch_shapes=[
            pltpu.VMEM((units, full), bf),
            pltpu.VMEM((units, full), bf),
            pltpu.VMEM((units, full), bf),
            pltpu.VMEM((HALVES, mp, size, width + LANES), bf),
            pltpu.VMEM((HALVES, mp, size, width), bf),
            pltpu.VMEM((HALVES, max(dp - 1, 1), mp, n * hr, width), bf),
            pltpu.VMEM((HALVES, max(mp - 1, 1), n * hr, width), bf),
            pltpu.VMEM((HALVES, n, hr, width), bf),
            pltpu.VMEM((HALVES, n, hr, width), bf),
            pltpu.VMEM((size, units), bf),
            pltpu.VMEM((LAYERS, HALVES, size, 1), f32),
            pltpu.VMEM((2, size, 1), f32),
            pltpu.VMEM((n * dp,) + share.shape, f32),
            dma((3,)),
            *pair(n, dp), *pair(HALVES, n, PARTS), *pair(HALVES, n, PARTS),
            *pair(HALVES, n, PARTS, mp), *pair(HALVES, n, PARTS, mp, dp),
            *pair(HALVES, mp, dp), *pair(HALVES, n, PARTS, mp),
            *pair(HALVES, n, PARTS), *pair(HALVES, n, PARTS),
        ],
        compiler_params=pltpu.CompilerParams(
            collective_id=0, has_side_effects=True, vmem_limit_bytes=67043328
        ),
    )(current, gain, share, w_gate, w_up, w_down)


def body(hidden_in, norm_gain, expert_ids, gate_counts, exit_layer, w_gate, w_up, w_down):
    n, dp, mp = lax.axis_size("expert"), lax.axis_size("dp"), lax.axis_size("mp")
    rows = hidden_in.shape[0]
    expert_range = jnp.arange(n, dtype=jnp.int32)
    counts = gate_counts.astype(jnp.float32)
    gate_share = counts / jnp.sum(counts, axis=2, keepdims=True)
    active = exit_layer[None, :] > jnp.arange(LAYERS, dtype=jnp.int32)[:, None]
    matched = (expert_ids[..., None] == expert_range) & active[:, :, None, None]
    share = jnp.sum(jnp.where(matched, gate_share[..., None], jnp.float32(0.0)), axis=2)
    share = share.transpose(0, 2, 1).reshape(LAYERS * n, rows)
    share = jnp.pad(share, ((0, -(LAYERS * n) % 8), (0, -rows % 128)))
    return stack(n, dp, mp, hidden_in, norm_gain, share, w_gate, w_up, w_down)


def solution(mesh):
    in_specs = (
        P(("groups", "expert", "dp"), "mp"),
        P(None, "mp"),
        P(None, ("groups", "expert", "dp"), None),
        P(None, ("groups", "expert", "dp"), None),
        P(("groups", "expert", "dp")),
        P(None, "expert", ("mp", "dp"), None),
        P(None, "expert", ("mp", "dp"), None),
        P(None, "expert", ("mp", "dp"), None),
    )
    out_specs = P(("groups", "expert", "dp"), "mp")
    return jax.shard_map(body, mesh=mesh, in_specs=in_specs, out_specs=out_specs, check_vma=False)
```

```python
import functools

import jax
import jax.numpy as jnp
from jax import lax
from jax.experimental import pallas as pl
from jax.experimental.pallas import tpu as pltpu
from jax.sharding import PartitionSpec as P

LAYERS = 2
HALVES = 2
PARTS = 2
LANES = 128

norm_floor = 0.1
MESH = pl.DeviceIdType.MESH
CHUNK = 16


def tile_of(length, best):
    tile = best
    while tile >= 128:
        if length % tile == 0:
            return tile
        tile //= 2
    return length


def stack_kernel(
    n, dp, mp,
    cur_ref, gain_ref, ids_ref, counts_ref, exit_ref, wg_hbm, wu_hbm, wd_hbm, out_ref,
    wg, wu, wd, xg, p, rd, xr, rzu, rzd, hid, col, inv, shares,
    w_sem, sh_s, sh_r, zu_s, zu_r, zd_s, zd_r, x_s, x_r, d_s, d_r,
    sw_s, sw_r, bx_s, bx_r, bu_s, bu_r, bd_s, bd_r,
):
    rows, width = cur_ref.shape
    full = width * mp
    units = wg.shape[0]
    hr = rows // HALVES
    pr = hr // PARTS
    core_rows = n * hr
    size = dp * core_rows
    e, m, d = lax.axis_index("expert"), lax.axis_index("mp"), lax.axis_index("dp")
    tile = tile_of(units, 256)
    steps = units // tile
    ctile = tile_of(width, 1024)
    csteps = width // ctile
    contract = (((1,), (1,)), ((), ()))

    def part(r):
        return lax.rem(m - r + mp, mp)

    def ahead(r):
        return {"mp": lax.rem(m + r, mp)}

    def core(k):
        return lax.rem(d + k, dp)

    place_of = {k: e + k for k in range(1 - n, n)}
    has = {k: (e + k <= n - 1 if k > 0 else e + k >= 0) for k in range(1 - n, n) if k}
    below, above = e > 0, e < n - 1
    up_z, down_z = {"expert": lax.rem(e + 1, n)}, {"expert": lax.rem(e + n - 1, n)}

    def remote(src, dst, ss, rs, dev):
        return pltpu.make_async_remote_copy(
            src_ref=src, dst_ref=dst, send_sem=ss, recv_sem=rs, device_id=dev, device_id_type=MESH
        )

    def weight(layer_idx, i):
        src, dst = ((wg_hbm, wg), (wu_hbm, wu), (wd_hbm, wd))[i]
        return pltpu.make_async_copy(src.at[layer_idx, 0], dst, w_sem.at[i])

    def row_of(c, blk, j=0):
        return pl.multiple_of((c * n + blk) * hr + j * pr, pr)

    def block_ref(h, blk, j, c, q):
        return xg.at[h, q, pl.ds(row_of(c, blk, j), pr)]

    def zu(h, s, j, blk):
        ref = block_ref(h, blk, j, d, m)
        return remote(ref, ref, zu_s.at[h], zu_r.at[h, s - 1, j], up_z)

    def zd(h, s, j, blk):
        ref = block_ref(h, blk, j, d, m)
        return remote(ref, ref, zd_s.at[h], zd_r.at[h, s - 1, j], down_z)

    def xm(h, blk, r, ref):
        return remote(ref, ref, x_s.at[h, r - 1], x_r.at[h, blk, r - 1], ahead(r))

    def dc(h, k, ref):
        return remote(ref, ref, d_s.at[h, k - 1], d_r.at[h, k - 1], {"dp": core(k)})

    def core_ref(h, c, q, first=0, count=n):
        at = pl.ds(pl.multiple_of(c * core_rows + first * hr, hr), count * hr)
        return xg.at[h, :, at] if q is None else xg.at[h, q, at]

    def spread(h, j, blk):
        for r in range(1, mp):
            xm(h, blk, r, block_ref(h, blk, j, d, m)).start()
        to_core(h, block_ref(h, blk, j, d, m))

    def to_core(h, ref):
        for k in range(1, dp):
            dc(h, k, ref).start()

    def own_z(h, j):
        pl.when(above)(lambda: zu(h, 1, j, e).start())
        pl.when(below)(lambda: zd(h, 1, j, e).start())

    def z_step(h, s, j):
        low, high = place_of[-s], place_of[s]

        def from_below():
            zu(h, s, j, low).wait_recv()
            if s + 1 < n:
                pl.when(above)(lambda: zu(h, s + 1, j, low).start())
            spread(h, j, low)

        def from_above():
            zd(h, s, j, high).wait_recv()
            if s + 1 < n:
                pl.when(below)(lambda: zd(h, s + 1, j, high).start())
            spread(h, j, high)

        pl.when(has[-s])(from_below)
        pl.when(has[s])(from_above)

    def x_step(h, s):
        def take(blk):
            for r in range(1, mp):
                ref = xg.at[h, part(r), pl.ds(row_of(d, blk), hr)]
                xm(h, blk, r, ref).wait_recv()
                to_core(h, ref)

        if s == 0:
            take(e)
        else:
            pl.when(has[-s])(lambda: take(place_of[-s]))
            pl.when(has[s])(lambda: take(place_of[s]))

    def core_done(h):
        for k in range(1, dp):
            dc(h, k, core_ref(h, core(dp - k), None)).wait_recv()

    def gather_sent(h):
        for k in range(1, dp):
            dc(h, k, core_ref(h, d, None)).wait_send()
        for r in range(1, mp):
            xm(h, e, r, core_ref(h, d, m)).wait_send()
        for i in range(n):
            def done(i=i):
                if i < n - 1:
                    ref = core_ref(h, d, m, 0, i + 1)
                    remote(ref, ref, zu_s.at[h], zu_r.at[h, 0, 0], up_z).wait_send()
                if i > 0:
                    ref = core_ref(h, d, m, i, n - i)
                    remote(ref, ref, zd_s.at[h], zd_r.at[h, 0, 0], down_z).wait_send()

            pl.when(e == i)(done)

    def own_rows(h, layer_idx, current):
        gain = gain_ref[...].astype(jnp.float32)[layer_idx:layer_idx + 1, :]
        lanes = lax.broadcasted_iota(jnp.int32, (CHUNK, LANES), 1)

        def chunk(i, _):
            at = pl.ds(pl.multiple_of(h * hr + i * CHUNK, CHUNK), CHUNK)
            v = current[at, :].astype(jnp.float32)
            left = jnp.sum(v * v, axis=1, keepdims=True)
            tail = jnp.zeros((CHUNK, LANES), jnp.float32)
            for lane in range(3):
                held = left.astype(jnp.bfloat16).astype(jnp.float32)
                tail = jnp.where(lanes == lane, held, tail)
                left = left - held
            to = pl.ds(pl.multiple_of(row_of(d, e) + i * CHUNK, CHUNK), CHUNK)
            xg[h, m, to, 0:width] = (v * gain).astype(jnp.bfloat16)
            xg[h, m, to, width:width + LANES] = tail.astype(jnp.bfloat16)
            return 0

        lax.fori_loop(0, hr // CHUNK, chunk, 0)

    def scales(h, layer_idx):
        total = jnp.zeros((size, 1), jnp.float32)
        for q in range(mp):
            tail = xg[h, q, :, width:width + LANES].astype(jnp.float32)
            total = total + jnp.sum(tail, axis=1, keepdims=True)
        scale = lax.rsqrt(total / full + norm_floor)
        inv[0] = scale
        inv[1] = scale * col[layer_idx, h]

    def hidden(h, layer_idx, events):
        def step(t, _):
            at = pl.ds(pl.multiple_of(t * tile, tile), tile)
            g = u = None
            for q in range(mp):
                a = xg[h, q, :, 0:width]
                wide = slice(q * width, (q + 1) * width)
                gq = lax.dot_general(a, wg[at, wide], contract, preferred_element_type=jnp.float32)
                uq = lax.dot_general(a, wu[at, wide], contract, preferred_element_type=jnp.float32)
                g, u = (gq, uq) if q == 0 else (g + gq, u + uq)
            g = g * inv[0]
            y = g / (1.0 + jnp.exp(-g)) * (u * inv[1])
            hid[:, at] = y.astype(jnp.bfloat16)
            for place, run in events:
                if steps == 1:
                    run()
                else:
                    pl.when(t == min(place * steps // 7, steps - 1))(run)
            return 0

        if steps == 1:
            step(0, 0)
        else:
            lax.fori_loop(0, steps, step, 0)

    def project(h, r, events=()):
        def step(t, _):
            q = part(r)
            off = pl.multiple_of(t * ctile, ctile)
            wide = pl.ds(pl.multiple_of(q * width + t * ctile, ctile), ctile)
            y = jnp.dot(hid[...], wd[:, wide], preferred_element_type=jnp.float32)
            p[h, q, :, pl.ds(off, ctile)] = y.astype(jnp.bfloat16)
            for k in range(1, dp):
                swap(h, r, k, pl.ds(off, ctile)).start()
            for place, run in events:
                pl.when(t == min(place, csteps - 1))(run)
            return 0

        lax.fori_loop(0, csteps, step, 0)

    def swap(h, r, k, at=None):
        q = part(r)
        rows_at = pl.ds(pl.multiple_of(core(k) * core_rows, core_rows), core_rows)
        src, dst = p.at[h, q, rows_at], rd.at[h, k - 1, q]
        if at is not None:
            src, dst = p.at[h, q, rows_at, at], rd.at[h, k - 1, q, :, at]
        return remote(src, dst, sw_s.at[h, r, k - 1], sw_r.at[h, r, k - 1], {"dp": core(k)})

    def swap_wait(h, r):
        for k in range(1, dp):
            swap(h, r, k).wait_recv()

    def chunks(j, count, run):
        def chunk(i, _):
            run(pl.multiple_of(j * pr + i * CHUNK, CHUNK))
            return 0

        if count == CHUNK:
            chunk(0, 0)
        else:
            lax.fori_loop(0, count // CHUNK, chunk, 0)

    def with_cores(h, q, blk, off):
        at = pl.ds(pl.multiple_of(row_of(d, blk) + off, CHUNK), CHUNK)
        other = pl.ds(pl.multiple_of(blk * hr + off, CHUNK), CHUNK)
        v = p[h, q, at, :].astype(jnp.float32)
        for k in range(1, dp):
            v = v + rd[h, k - 1, q, other, :].astype(jnp.float32)
        return at, other, v

    def bx(h, blk, j, r):
        src = p.at[h, part(r), pl.ds(row_of(d, blk, j), pr)]
        dst = xr.at[h, r - 1, pl.ds(pl.multiple_of(blk * hr + j * pr, pr), pr)]
        return remote(src, dst, bx_s.at[h, r - 1], bx_r.at[h, blk, j, r - 1], {"mp": part(r)})

    def by_distance(k, run):
        if k == 0:
            run(e)
        else:
            pl.when(has[k])(lambda: run(place_of[k]))
            pl.when(has[-k])(lambda: run(place_of[-k]))

    def back_x(h, k):
        def run(blk):
            for j in range(PARTS):
                for r in range(1, mp):
                    def put(off, q=part(r)):
                        at, _, v = with_cores(h, q, blk, off)
                        p[h, q, at, :] = v.astype(jnp.bfloat16)

                    chunks(j, pr, put)
                    bx(h, blk, j, r).start()

        by_distance(k, run)

    def bu(h, blk, j):
        src = p.at[h, m, pl.ds(row_of(d, blk, j), pr)]
        dst = rzu.at[h, blk, pl.ds(j * pr, pr)]
        return remote(src, dst, bu_s.at[h], bu_r.at[h, blk - 1, j], up_z)

    def bd(h, blk, j):
        src = p.at[h, m, pl.ds(row_of(d, blk, j), pr)]
        dst = rzd.at[h, blk, pl.ds(j * pr, pr)]
        return remote(src, dst, bd_s.at[h], bd_r.at[h, blk, j], down_z)

    def out_ref_of(h, q, first=0, count=n):
        return p.at[h, q, pl.ds(pl.multiple_of(d * core_rows + first * hr, hr), count * hr)]

    def home_sent(h):
        for r in range(mp):
            for k in range(1, dp):
                swap(h, r, k).wait_send()
        for r in range(1, mp):
            ref = out_ref_of(h, part(r))
            remote(ref, ref, bx_s.at[h, r - 1], bx_r.at[h, 0, 0, r - 1], {"mp": part(r)}).wait_send()
        for i in range(n):
            def done(i=i):
                if i < n - 1:
                    ref = out_ref_of(h, m, i + 1, n - 1 - i)
                    remote(ref, ref, bu_s.at[h], bu_r.at[h, 0, 0], up_z).wait_send()
                if i > 0:
                    ref = out_ref_of(h, m, 0, i)
                    remote(ref, ref, bd_s.at[h], bd_r.at[h, 0, 0], down_z).wait_send()

            pl.when(e == i)(done)

    def gathered(h, blk, off):
        at, other, v = with_cores(h, m, blk, off)
        for r in range(1, mp):
            v = v + xr[h, r - 1, other, :].astype(jnp.float32)
        return at, v

    def plain(h, blk, j):
        def put(off):
            at, v = gathered(h, blk, off)
            p[h, m, at, :] = v.astype(jnp.bfloat16)

        chunks(j, pr, put)

    def joined(h, blk, j, incoming):
        def put(off):
            at, v = gathered(h, blk, off)
            v = v + incoming[h, blk, pl.ds(off, CHUNK), :].astype(jnp.float32)
            p[h, m, at, :] = v.astype(jnp.bfloat16)

        chunks(j, pr, put)

    def back_z(h, k, j):
        def along(blk, copy, inner, incoming):
            for r in range(1, mp):
                bx(h, blk, j, r).wait_recv()

            @pl.when(inner)
            def _():
                copy(h, blk, j).wait_recv()
                joined(h, blk, j, incoming)

            pl.when(jnp.logical_not(inner))(lambda: plain(h, blk, j))
            copy(h, blk, j).start()

        pl.when(has[k])(lambda: along(place_of[k], bu, below, rzu))
        pl.when(has[-k])(lambda: along(place_of[-k], bd, above, rzd))

    def arrive(h, current):
        for j in range(PARTS):
            for r in range(1, mp):
                bx(h, e, j, r).wait_recv()
            pl.when(below)(lambda j=j: bu(h, e, j).wait_recv())
            pl.when(above)(lambda j=j: bd(h, e, j).wait_recv())

        def finish(sources):
            def put(off):
                _, v = gathered(h, e, off)
                for ref in sources:
                    v = v + ref[h, e, pl.ds(off, CHUNK), :].astype(jnp.float32)
                at = pl.ds(pl.multiple_of(h * hr + off, CHUNK), CHUNK)
                out_ref[at, :] = (current[at, :].astype(jnp.float32) + v).astype(jnp.bfloat16)

            chunks(0, hr, put)

        if n == 1:
            finish([])
        else:
            pl.when(jnp.logical_not(below))(lambda: finish([rzd]))
            pl.when(jnp.logical_not(above))(lambda: finish([rzu]))
            if n > 2:
                pl.when(jnp.logical_and(below, above))(lambda: finish([rzu, rzd]))

    slot = d * n + e
    others = [(k, c) for k in range(n) for c in range(dp) if k + c > 0]

    def share_copies():
        ref = shares.at[slot]
        return [remote(ref, ref, sh_s.at[0], sh_r.at[0],
                       {"expert": lax.rem(e + k, n), "dp": core(c)}) for k, c in others]

    def own_shares():
        tall = shares.shape[1]
        line = lax.broadcasted_iota(jnp.int32, (tall, rows), 0)
        tile = jnp.zeros((tall, rows), jnp.float32)
        for layer_idx in range(LAYERS):
            count = counts_ref[layer_idx].astype(jnp.float32)
            named = ids_ref[layer_idx] + layer_idx * n
            whole = jnp.sum(count, axis=0, keepdims=True)
            part_of = jnp.where(exit_ref[...] > layer_idx, count / whole, 0.0)
            for choice in range(count.shape[0]):
                hit = line == named[choice:choice + 1]
                tile = tile + jnp.where(hit, part_of[choice:choice + 1], 0.0)
        shares[slot] = jnp.zeros(shares.shape[1:], jnp.float32)
        shares[slot, :, 0:rows] = tile

    def columns():
        ref = shares.at[pl.ds(0, len(others))]
        if others:
            remote(ref, ref, sh_s.at[0], sh_r.at[0], {"expert": e}).wait_recv()
        lanes = lax.broadcasted_iota(jnp.int32, (shares.shape[2], shares.shape[1]), 1)
        for place in range(n * dp):
            tokens = shares[place].T
            for layer_idx in range(LAYERS):
                picked = jnp.sum(
                    jnp.where(lanes == layer_idx * n + e, tokens, 0.0), axis=1, keepdims=True
                )
                for h in range(HALVES):
                    col[layer_idx, h, place * hr:(place + 1) * hr, :] = picked[h * hr:(h + 1) * hr]

    barrier = pltpu.get_barrier_semaphore()
    peers = [ahead(r) for r in range(1, mp)]
    peers += [{"expert": lax.rem(e + k, n), "dp": core(c)} for k, c in others]
    for dev in peers:
        pl.semaphore_signal(barrier, inc=1, device_id=dev, device_id_type=MESH)
    own_rows(0, 0, cur_ref)
    own_shares()
    pl.semaphore_wait(barrier, len(peers))

    both = range(PARTS)
    far = list(range(n - 1, 0, -1))

    def start_own(h):
        for j in both:
            own_z(h, j)
            spread(h, j, e)

    def z_all(h, s):
        for j in both:
            z_step(h, s, j)

    def back_all(h, k):
        for j in both:
            back_z(h, k, j)

    def back_x_all(h):
        for r in range(1, mp):
            swap_wait(h, r)
        for k in far + [0]:
            back_x(h, k)

    for layer_idx in range(LAYERS):
        if layer_idx == 0:
            start_own(0)
            for copy in share_copies():
                copy.start()
            own_rows(1, 0, cur_ref)
            for j in both:
                spread(1, j, e)
            for s in range(1, n):
                z_all(0, s)
                if s == 1:
                    for i in range(3):
                        weight(0, i).start()
                if s == max(n - 2, 1):
                    for j in both:
                        own_z(1, j)
            columns()
        else:
            arrive(0, cur_ref)
            own_rows(0, layer_idx, out_ref)
            start_own(0)
            swap_wait(1, 0)
            for k in far:
                back_all(1, k)
                z_all(0, n - k)
            arrive(1, cur_ref)
            own_rows(1, layer_idx, out_ref)
            start_own(1)
        for s in range(n - 1):
            x_step(0, s)
        if n > 1:
            z_all(1, 1)
        x_step(0, n - 1)
        core_done(0)
        scales(0, layer_idx)
        weight(layer_idx, 0).wait()
        weight(layer_idx, 1).wait()
        events = [(2 * s - 2, lambda s=s: z_all(1, s)) for s in range(2, n)]
        events += [(5, lambda s=s: x_step(1, s)) for s in range(n - 2)]
        hidden(0, layer_idx, events)
        weight(layer_idx, 2).wait()
        if layer_idx > 0:
            home_sent(0)
        gather_sent(0)
        for r in range(1, mp):
            project(0, r)
        if n > 1:
            x_step(1, n - 2)
        project(0, 0, [(0, lambda: back_x_all(0))])
        x_step(1, n - 1)
        core_done(1)
        scales(1, layer_idx)
        rest = [(k, j) for k in far for j in both]
        late = rest[-1:]
        spots = [0, 1, 3, 4, 6]
        events = [(0, lambda: swap_wait(0, 0))]
        events += [
            (spots[min(i, 4)], lambda k=k, j=j: back_z(0, k, j)) for i, (k, j) in enumerate(rest[:-1])
        ]
        hidden(1, layer_idx, events)
        if layer_idx + 1 < LAYERS:
            weight(layer_idx + 1, 0).start()
            weight(layer_idx + 1, 1).start()
        if layer_idx > 0:
            home_sent(1)
        gather_sent(1)
        for r in range(1, mp):
            project(1, r)
        for k, j in late:
            back_z(0, k, j)
        project(1, 0, [(0, lambda: back_x_all(1))])
        if layer_idx + 1 < LAYERS:
            weight(layer_idx + 1, 2).start()
    arrive(0, out_ref)
    swap_wait(1, 0)
    for k in far:
        back_all(1, k)
    arrive(1, out_ref)
    for h in range(HALVES):
        home_sent(h)
    if others:
        ref = shares.at[pl.ds(0, len(others))]
        remote(ref, ref, sh_s.at[0], sh_r.at[0], {"expert": e}).wait_send()


def stack(n, dp, mp, current, gain, ids, counts, exits, w_gate, w_up, w_down):
    rows, width = current.shape
    units, full = w_gate.shape[2:]
    hr = rows // HALVES
    size = n * dp * hr
    bf, f32, dma = jnp.bfloat16, jnp.float32, pltpu.SemaphoreType.DMA
    vmem = pl.BlockSpec(memory_space=pltpu.VMEM)
    hbm = pl.BlockSpec(memory_space=pl.ANY)
    cores, sides, hops = max(dp - 1, 1), max(mp - 1, 1), max(n - 1, 1)
    share_shape = (n * dp, LAYERS * n + -(LAYERS * n) % 8, rows + -rows % 128)

    def pair(*shape):
        return [dma(shape), dma(shape)]

    return pl.pallas_call(
        functools.partial(stack_kernel, n, dp, mp),
        out_shape=jax.ShapeDtypeStruct((rows, width), bf),
        in_specs=[vmem, vmem, vmem, vmem, vmem, hbm, hbm, hbm],
        out_specs=vmem,
        scratch_shapes=[
            pltpu.VMEM((units, full), bf),
            pltpu.VMEM((units, full), bf),
            pltpu.VMEM((units, full), bf),
            pltpu.VMEM((HALVES, mp, size, width + LANES), bf),
            pltpu.VMEM((HALVES, mp, size, width), bf),
            pltpu.VMEM((HALVES, cores, mp, n * hr, width), bf),
            pltpu.VMEM((HALVES, sides, n * hr, width), bf),
            pltpu.VMEM((HALVES, n, hr, width), bf),
            pltpu.VMEM((HALVES, n, hr, width), bf),
            pltpu.VMEM((size, units), bf),
            pltpu.VMEM((LAYERS, HALVES, size, 1), f32),
            pltpu.VMEM((2, size, 1), f32),
            pltpu.VMEM(share_shape, f32),
            dma((3,)), *pair(1),
            dma((HALVES,)), dma((HALVES, hops, PARTS)), dma((HALVES,)), dma((HALVES, hops, PARTS)),
            dma((HALVES, sides)), dma((HALVES, n, sides)), *pair(HALVES, cores),
            *pair(HALVES, mp, cores), dma((HALVES, sides)), dma((HALVES, n, PARTS, sides)),
            dma((HALVES,)), dma((HALVES, hops, PARTS)), dma((HALVES,)), dma((HALVES, hops, PARTS)),
        ],
        compiler_params=pltpu.CompilerParams(
            collective_id=0, has_side_effects=True, vmem_limit_bytes=67043328
        ),
    )(current, gain, ids, counts, exits, w_gate, w_up, w_down)


def body(hidden_in, norm_gain, expert_ids, gate_counts, exit_layer, w_gate, w_up, w_down):
    n, dp, mp = lax.axis_size("expert"), lax.axis_size("dp"), lax.axis_size("mp")
    return stack(
        n, dp, mp, hidden_in, norm_gain, expert_ids.transpose(0, 2, 1),
        gate_counts.transpose(0, 2, 1), exit_layer[None, :], w_gate, w_up, w_down,
    )


def solution(mesh):
    in_specs = (
        P(("groups", "expert", "dp"), "mp"),
        P(None, "mp"),
        P(None, ("groups", "expert", "dp"), None),
        P(None, ("groups", "expert", "dp"), None),
        P(("groups", "expert", "dp")),
        P(None, "expert", ("mp", "dp"), None),
        P(None, "expert", ("mp", "dp"), None),
        P(None, "expert", ("mp", "dp"), None),
    )
    out_specs = P(("groups", "expert", "dp"), "mp")
    return jax.shard_map(body, mesh=mesh, in_specs=in_specs, out_specs=out_specs, check_vma=False)
```

```python
import functools

import jax
import jax.numpy as jnp
from jax import lax
from jax.experimental import pallas as pl
from jax.experimental.pallas import tpu as pltpu
from jax.sharding import PartitionSpec as P

LAYERS = 2
HALVES = 2
PARTS = 2
LANES = 128

norm_floor = 0.1
MESH = pl.DeviceIdType.MESH
CHUNK = 16


def tile_of(length, best):
    tile = best
    while tile >= 128:
        if length % tile == 0:
            return tile
        tile //= 2
    return length


def stack_kernel(
    n, dp, mp,
    cur_ref, gain_ref, ids_ref, counts_ref, exit_ref, wg_hbm, wu_hbm, wd_hbm, out_ref,
    wg, wu, wd, xg, p, rd, xr, rzu, rzd, rzf, hid, col, inv, shares,
    w_sem, sh_s, sh_r, zu_s, zu_r, zd_s, zd_r, x_s, x_r, d_s, d_r,
    sw_s, sw_r, bx_s, bx_r, bu_s, bu_r, bd_s, bd_r, bf_s, bf_r,
):
    rows, width = cur_ref.shape
    full = width * mp
    units = wg.shape[0]
    hr = rows // HALVES
    pr = hr // PARTS
    core_rows = n * hr
    size = dp * core_rows
    e, m, d = lax.axis_index("expert"), lax.axis_index("mp"), lax.axis_index("dp")
    tile = tile_of(units, 256)
    steps = units // tile
    ctile = tile_of(width, 1024)
    csteps = width // ctile
    contract = (((1,), (1,)), ((), ()))

    def part(r):
        return lax.rem(m - r + mp, mp)

    def ahead(r):
        return {"mp": lax.rem(m + r, mp)}

    def core(k):
        return lax.rem(d + k, dp)

    place_of = {k: e + k for k in range(1 - n, n)}
    has = {k: (e + k <= n - 1 if k > 0 else e + k >= 0) for k in range(1 - n, n) if k}
    below, above = e > 0, e < n - 1
    direct = n > 3
    up_z, down_z = {"expert": lax.rem(e + 1, n)}, {"expert": lax.rem(e + n - 1, n)}

    def remote(src, dst, ss, rs, dev):
        return pltpu.make_async_remote_copy(
            src_ref=src, dst_ref=dst, send_sem=ss, recv_sem=rs, device_id=dev, device_id_type=MESH
        )

    def weight(layer_idx, i):
        src, dst = ((wg_hbm, wg), (wu_hbm, wu), (wd_hbm, wd))[i]
        return pltpu.make_async_copy(src.at[layer_idx, 0], dst, w_sem.at[i])

    def row_of(c, blk, j=0):
        return pl.multiple_of((c * n + blk) * hr + j * pr, pr)

    def block_ref(h, blk, j, c, q):
        return xg.at[h, q, pl.ds(row_of(c, blk, j), pr)]

    def zu(h, s, j, blk):
        ref = block_ref(h, blk, j, d, m)
        return remote(ref, ref, zu_s.at[h], zu_r.at[h, s - 1, j], up_z)

    def zd(h, s, j, blk):
        ref = block_ref(h, blk, j, d, m)
        return remote(ref, ref, zd_s.at[h], zd_r.at[h, s - 1, j], down_z)

    def xm(h, blk, r, ref):
        return remote(ref, ref, x_s.at[h, r - 1], x_r.at[h, blk, r - 1], ahead(r))

    def dc(h, k, ref):
        return remote(ref, ref, d_s.at[h, k - 1], d_r.at[h, k - 1], {"dp": core(k)})

    def core_ref(h, c, q, first=0, count=n):
        at = pl.ds(pl.multiple_of(c * core_rows + first * hr, hr), count * hr)
        return xg.at[h, :, at] if q is None else xg.at[h, q, at]

    def spread(h, j, blk):
        for r in range(1, mp):
            xm(h, blk, r, block_ref(h, blk, j, d, m)).start()
        to_core(h, block_ref(h, blk, j, d, m))

    def to_core(h, ref):
        for k in range(1, dp):
            dc(h, k, ref).start()

    def own_z(h, j):
        pl.when(above)(lambda: zu(h, 1, j, e).start())
        pl.when(below)(lambda: zd(h, 1, j, e).start())

    def z_step(h, s, j):
        low, high = place_of[-s], place_of[s]

        def from_below():
            zu(h, s, j, low).wait_recv()
            if s + 1 < n:
                pl.when(above)(lambda: zu(h, s + 1, j, low).start())
            spread(h, j, low)

        def from_above():
            zd(h, s, j, high).wait_recv()
            if s + 1 < n:
                pl.when(below)(lambda: zd(h, s + 1, j, high).start())
            spread(h, j, high)

        pl.when(has[-s])(from_below)
        pl.when(has[s])(from_above)

    def x_step(h, s):
        def take(blk):
            for r in range(1, mp):
                ref = xg.at[h, part(r), pl.ds(row_of(d, blk), hr)]
                xm(h, blk, r, ref).wait_recv()
                to_core(h, ref)

        if s == 0:
            take(e)
        else:
            pl.when(has[-s])(lambda: take(place_of[-s]))
            pl.when(has[s])(lambda: take(place_of[s]))

    def core_done(h):
        for k in range(1, dp):
            dc(h, k, core_ref(h, core(dp - k), None)).wait_recv()

    def gather_sent(h):
        for k in range(1, dp):
            dc(h, k, core_ref(h, d, None)).wait_send()
        for r in range(1, mp):
            xm(h, e, r, core_ref(h, d, m)).wait_send()
        for i in range(n):
            def done(i=i):
                if i < n - 1:
                    ref = core_ref(h, d, m, 0, i + 1)
                    remote(ref, ref, zu_s.at[h], zu_r.at[h, 0, 0], up_z).wait_send()
                if i > 0:
                    ref = core_ref(h, d, m, i, n - i)
                    remote(ref, ref, zd_s.at[h], zd_r.at[h, 0, 0], down_z).wait_send()

            pl.when(e == i)(done)

    def own_rows(h, layer_idx, current):
        gain = gain_ref[...].astype(jnp.float32)[layer_idx:layer_idx + 1, :]
        lanes = lax.broadcasted_iota(jnp.int32, (CHUNK, LANES), 1)

        def chunk(i, _):
            at = pl.ds(pl.multiple_of(h * hr + i * CHUNK, CHUNK), CHUNK)
            v = current[at, :].astype(jnp.float32)
            left = jnp.sum(v * v, axis=1, keepdims=True)
            tail = jnp.zeros((CHUNK, LANES), jnp.float32)
            for lane in range(3):
                held = left.astype(jnp.bfloat16).astype(jnp.float32)
                tail = jnp.where(lanes == lane, held, tail)
                left = left - held
            to = pl.ds(pl.multiple_of(row_of(d, e) + i * CHUNK, CHUNK), CHUNK)
            xg[h, m, to, 0:width] = (v * gain).astype(jnp.bfloat16)
            xg[h, m, to, width:width + LANES] = tail.astype(jnp.bfloat16)
            return 0

        lax.fori_loop(0, hr // CHUNK, chunk, 0)

    def scales(h, layer_idx):
        total = jnp.zeros((size, 1), jnp.float32)
        for q in range(mp):
            tail = xg[h, q, :, width:width + LANES].astype(jnp.float32)
            total = total + jnp.sum(tail, axis=1, keepdims=True)
        scale = lax.rsqrt(total / full + norm_floor)
        inv[0] = scale
        inv[1] = scale * col[layer_idx, h]

    def hidden(h, layer_idx, events):
        def step(t, _):
            at = pl.ds(pl.multiple_of(t * tile, tile), tile)
            g = u = None
            for q in range(mp):
                a = xg[h, q, :, 0:width]
                wide = slice(q * width, (q + 1) * width)
                gq = lax.dot_general(a, wg[at, wide], contract, preferred_element_type=jnp.float32)
                uq = lax.dot_general(a, wu[at, wide], contract, preferred_element_type=jnp.float32)
                g, u = (gq, uq) if q == 0 else (g + gq, u + uq)
            g = g * inv[0]
            y = g / (1.0 + jnp.exp(-g)) * (u * inv[1])
            hid[:, at] = y.astype(jnp.bfloat16)
            for place, run in events:
                if steps == 1:
                    run()
                else:
                    pl.when(t == min(place * steps // 7, steps - 1))(run)
            return 0

        if steps == 1:
            step(0, 0)
        else:
            lax.fori_loop(0, steps, step, 0)

    def project(h, r, events=()):
        def step(t, _):
            q = part(r)
            off = pl.multiple_of(t * ctile, ctile)
            wide = pl.ds(pl.multiple_of(q * width + t * ctile, ctile), ctile)
            y = jnp.dot(hid[...], wd[:, wide], preferred_element_type=jnp.float32)
            p[h, q, :, pl.ds(off, ctile)] = y.astype(jnp.bfloat16)
            for k in range(1, dp):
                swap(h, r, k, pl.ds(off, ctile)).start()
            for place, run in events:
                pl.when(t == min(place, csteps - 1))(run)
            return 0

        lax.fori_loop(0, csteps, step, 0)

    def swap(h, r, k, at=None):
        q = part(r)
        rows_at = pl.ds(pl.multiple_of(core(k) * core_rows, core_rows), core_rows)
        src, dst = p.at[h, q, rows_at], rd.at[h, k - 1, q]
        if at is not None:
            src, dst = p.at[h, q, rows_at, at], rd.at[h, k - 1, q, :, at]
        return remote(src, dst, sw_s.at[h, r, k - 1], sw_r.at[h, r, k - 1], {"dp": core(k)})

    def swap_wait(h, r):
        for k in range(1, dp):
            swap(h, r, k).wait_recv()

    def chunks(j, count, run):
        def chunk(i, _):
            run(pl.multiple_of(j * pr + i * CHUNK, CHUNK))
            return 0

        if count == CHUNK:
            chunk(0, 0)
        else:
            lax.fori_loop(0, count // CHUNK, chunk, 0)

    def with_cores(h, q, blk, off):
        at = pl.ds(pl.multiple_of(row_of(d, blk) + off, CHUNK), CHUNK)
        other = pl.ds(pl.multiple_of(blk * hr + off, CHUNK), CHUNK)
        v = p[h, q, at, :].astype(jnp.float32)
        for k in range(1, dp):
            v = v + rd[h, k - 1, q, other, :].astype(jnp.float32)
        return at, other, v

    def bx(h, blk, j, r):
        src = p.at[h, part(r), pl.ds(row_of(d, blk, j), pr)]
        dst = xr.at[h, r - 1, pl.ds(pl.multiple_of(blk * hr + j * pr, pr), pr)]
        return remote(src, dst, bx_s.at[h, r - 1], bx_r.at[h, blk, j, r - 1], {"mp": part(r)})

    def by_distance(k, run):
        if k == 0:
            run(e)
        else:
            pl.when(has[k])(lambda: run(place_of[k]))
            pl.when(has[-k])(lambda: run(place_of[-k]))

    def back_x(h, k):
        def run(blk):
            for j in range(PARTS):
                for r in range(1, mp):
                    def put(off, q=part(r)):
                        at, _, v = with_cores(h, q, blk, off)
                        p[h, q, at, :] = v.astype(jnp.bfloat16)

                    chunks(j, pr, put)
                    bx(h, blk, j, r).start()

        by_distance(k, run)

    def bu(h, blk, j):
        src = p.at[h, m, pl.ds(row_of(d, blk, j), pr)]
        dst = rzu.at[h, blk, pl.ds(j * pr, pr)]
        return remote(src, dst, bu_s.at[h], bu_r.at[h, blk - 1, j], up_z)

    def bd(h, blk, j):
        src = p.at[h, m, pl.ds(row_of(d, blk, j), pr)]
        dst = rzd.at[h, blk, pl.ds(j * pr, pr)]
        return remote(src, dst, bd_s.at[h], bd_r.at[h, blk, j], down_z)

    def bf(h, blk, j):
        src = p.at[h, m, pl.ds(row_of(d, blk, j), pr)]
        dst = rzf.at[h, pl.ds(j * pr, pr)]
        return remote(src, dst, bf_s.at[h], bf_r.at[h, j], {"expert": n - 1 - e})

    def out_ref_of(h, q, first=0, count=n):
        return p.at[h, q, pl.ds(pl.multiple_of(d * core_rows + first * hr, hr), count * hr)]

    def home_sent(h):
        for r in range(mp):
            for k in range(1, dp):
                swap(h, r, k).wait_send()
        for r in range(1, mp):
            ref = out_ref_of(h, part(r))
            remote(ref, ref, bx_s.at[h, r - 1], bx_r.at[h, 0, 0, r - 1], {"mp": part(r)}).wait_send()
        for i in range(n):
            def done(i=i):
                edge = int(direct and i in (0, n - 1))
                if edge:
                    ref = out_ref_of(h, m, 0, 1)
                    remote(ref, ref, bf_s.at[h], bf_r.at[h, 0], {"expert": n - 1 - e}).wait_send()
                if i < n - 1:
                    ref = out_ref_of(h, m, i + 1, n - 1 - i - edge)
                    remote(ref, ref, bu_s.at[h], bu_r.at[h, 0, 0], up_z).wait_send()
                if i > 0:
                    ref = out_ref_of(h, m, edge, i - edge)
                    remote(ref, ref, bd_s.at[h], bd_r.at[h, 0, 0], down_z).wait_send()

            pl.when(e == i)(done)

    def gathered(h, blk, off):
        at, other, v = with_cores(h, m, blk, off)
        for r in range(1, mp):
            v = v + xr[h, r - 1, other, :].astype(jnp.float32)
        return at, v

    def plain(h, blk, j):
        def put(off):
            at, v = gathered(h, blk, off)
            p[h, m, at, :] = v.astype(jnp.bfloat16)

        chunks(j, pr, put)

    def joined(h, blk, j, incoming):
        def put(off):
            at, v = gathered(h, blk, off)
            v = v + incoming[h, blk, pl.ds(off, CHUNK), :].astype(jnp.float32)
            p[h, m, at, :] = v.astype(jnp.bfloat16)

        chunks(j, pr, put)

    def back_z(h, k, j):
        def along(blk, copy, inner, incoming):
            for r in range(1, mp):
                bx(h, blk, j, r).wait_recv()

            if direct and k >= n - 2:
                plain(h, blk, j)
            else:
                @pl.when(inner)
                def _():
                    copy(h, blk, j).wait_recv()
                    joined(h, blk, j, incoming)

                pl.when(jnp.logical_not(inner))(lambda: plain(h, blk, j))
            if direct and k == n - 1:
                bf(h, blk, j).start()
            else:
                copy(h, blk, j).start()

        pl.when(has[k])(lambda: along(place_of[k], bu, below, rzu))
        pl.when(has[-k])(lambda: along(place_of[-k], bd, above, rzd))

    def arrive(h, current):
        for j in range(PARTS):
            for r in range(1, mp):
                bx(h, e, j, r).wait_recv()
            pl.when(below)(lambda j=j: bu(h, e, j).wait_recv())
            pl.when(above)(lambda j=j: bd(h, e, j).wait_recv())
            if direct:
                pl.when(e == 0)(lambda j=j: bf(h, e, j).wait_recv())
                pl.when(e == n - 1)(lambda j=j: bf(h, e, j).wait_recv())

        def finish(sources, far_too=False):
            def put(off):
                _, v = gathered(h, e, off)
                if far_too:
                    v = v + rzf[h, pl.ds(off, CHUNK), :].astype(jnp.float32)
                for ref in sources:
                    v = v + ref[h, e, pl.ds(off, CHUNK), :].astype(jnp.float32)
                at = pl.ds(pl.multiple_of(h * hr + off, CHUNK), CHUNK)
                out_ref[at, :] = (current[at, :].astype(jnp.float32) + v).astype(jnp.bfloat16)

            chunks(0, hr, put)

        if n == 1:
            finish([])
        else:
            pl.when(jnp.logical_not(below))(lambda: finish([rzd], direct))
            pl.when(jnp.logical_not(above))(lambda: finish([rzu], direct))
            if n > 2:
                pl.when(jnp.logical_and(below, above))(lambda: finish([rzu, rzd]))

    slot = d * n + e
    others = [(k, c) for k in range(n) for c in range(dp) if k + c > 0]

    def share_copies():
        ref = shares.at[slot]
        return [remote(ref, ref, sh_s.at[0], sh_r.at[0],
                       {"expert": lax.rem(e + k, n), "dp": core(c)}) for k, c in others]

    def own_shares():
        tall = shares.shape[1]
        line = lax.broadcasted_iota(jnp.int32, (tall, rows), 0)
        tile = jnp.zeros((tall, rows), jnp.float32)
        for layer_idx in range(LAYERS):
            count = counts_ref[layer_idx].astype(jnp.float32)
            named = ids_ref[layer_idx] + layer_idx * n
            whole = jnp.sum(count, axis=0, keepdims=True)
            part_of = jnp.where(exit_ref[...] > layer_idx, count / whole, 0.0)
            for choice in range(count.shape[0]):
                hit = line == named[choice:choice + 1]
                tile = tile + jnp.where(hit, part_of[choice:choice + 1], 0.0)
        shares[slot] = jnp.zeros(shares.shape[1:], jnp.float32)
        shares[slot, :, 0:rows] = tile

    def columns():
        ref = shares.at[pl.ds(0, len(others))]
        if others:
            remote(ref, ref, sh_s.at[0], sh_r.at[0], {"expert": e}).wait_recv()
        lanes = lax.broadcasted_iota(jnp.int32, (shares.shape[2], shares.shape[1]), 1)
        for place in range(n * dp):
            tokens = shares[place].T
            for layer_idx in range(LAYERS):
                picked = jnp.sum(
                    jnp.where(lanes == layer_idx * n + e, tokens, 0.0), axis=1, keepdims=True
                )
                for h in range(HALVES):
                    col[layer_idx, h, place * hr:(place + 1) * hr, :] = picked[h * hr:(h + 1) * hr]

    barrier = pltpu.get_barrier_semaphore()
    peers = [ahead(r) for r in range(1, mp)]
    peers += [{"expert": lax.rem(e + k, n), "dp": core(c)} for k, c in others]
    for dev in peers:
        pl.semaphore_signal(barrier, inc=1, device_id=dev, device_id_type=MESH)
    own_rows(0, 0, cur_ref)
    own_shares()
    pl.semaphore_wait(barrier, len(peers))

    both = range(PARTS)
    far = list(range(n - 1, 0, -1))
    if direct:
        far[0:2] = [n - 2, n - 1]

    def start_own(h):
        for j in both:
            own_z(h, j)
            spread(h, j, e)

    def z_all(h, s):
        for j in both:
            z_step(h, s, j)

    def back_all(h, k):
        for j in both:
            back_z(h, k, j)

    def back_x_all(h):
        for r in range(1, mp):
            swap_wait(h, r)
        for k in far + [0]:
            back_x(h, k)

    for layer_idx in range(LAYERS):
        if layer_idx == 0:
            start_own(0)
            for copy in share_copies():
                copy.start()
            own_rows(1, 0, cur_ref)
            spread(1, 0, e)
            for s in range(1, n):
                z_all(0, s)
                if s == 1:
                    for j in both[1:]:
                        spread(1, j, e)
                    for i in range(3):
                        weight(0, i).start()
                if s == max(n - 2, 1):
                    for j in both:
                        own_z(1, j)
            columns()
        else:
            arrive(0, cur_ref)
            own_rows(0, layer_idx, out_ref)
            start_own(0)
            swap_wait(1, 0)
            for i, k in enumerate(far):
                back_all(1, k)
                z_all(0, i + 1)
            arrive(1, cur_ref)
            own_rows(1, layer_idx, out_ref)
            start_own(1)
        for s in range(n - 1):
            x_step(0, s)
        if n > 1:
            z_all(1, 1)
        x_step(0, n - 1)
        core_done(0)
        scales(0, layer_idx)
        weight(layer_idx, 0).wait()
        weight(layer_idx, 1).wait()
        events = [(3 * s - 4, lambda s=s: z_all(1, s)) for s in range(2, n)]
        events += [(5, lambda s=s: x_step(1, s)) for s in range(n - 2)]
        hidden(0, layer_idx, events)
        weight(layer_idx, 2).wait()
        if layer_idx > 0:
            home_sent(0)
        gather_sent(0)
        for r in range(1, mp):
            project(0, r)
        if n > 1:
            x_step(1, n - 2)
        last_x = [(0, lambda: x_step(1, n - 1))] if n > 1 else []
        project(0, 0, [(0, lambda: back_x_all(0))] + last_x)
        core_done(1)
        scales(1, layer_idx)
        rest = [(k, j) for k in far for j in both]
        late = rest[-1:]
        spots = [0, 1, 3, 4, 6]
        events = [(0, lambda: swap_wait(0, 0))]
        events += [
            (spots[min(i, 4)], lambda k=k, j=j: back_z(0, k, j)) for i, (k, j) in enumerate(rest[:-1])
        ]
        hidden(1, layer_idx, events)
        if layer_idx + 1 < LAYERS:
            weight(layer_idx + 1, 0).start()
            weight(layer_idx + 1, 1).start()
        if layer_idx > 0:
            home_sent(1)
        gather_sent(1)
        for r in range(1, mp):
            project(1, r)
        for k, j in late:
            back_z(0, k, j)
        project(1, 0, [(0, lambda: back_x_all(1))])
        if layer_idx + 1 < LAYERS:
            weight(layer_idx + 1, 2).start()
    arrive(0, out_ref)
    swap_wait(1, 0)
    for k in far:
        back_all(1, k)
    arrive(1, out_ref)
    for h in range(HALVES):
        home_sent(h)
    if others:
        ref = shares.at[pl.ds(0, len(others))]
        remote(ref, ref, sh_s.at[0], sh_r.at[0], {"expert": e}).wait_send()


def stack(n, dp, mp, current, gain, ids, counts, exits, w_gate, w_up, w_down):
    rows, width = current.shape
    units, full = w_gate.shape[2:]
    hr = rows // HALVES
    size = n * dp * hr
    bf, f32, dma = jnp.bfloat16, jnp.float32, pltpu.SemaphoreType.DMA
    vmem = pl.BlockSpec(memory_space=pltpu.VMEM)
    hbm = pl.BlockSpec(memory_space=pl.ANY)
    cores, sides, hops = max(dp - 1, 1), max(mp - 1, 1), max(n - 1, 1)
    share_shape = (n * dp, LAYERS * n + -(LAYERS * n) % 8, rows + -rows % 128)

    def pair(*shape):
        return [dma(shape), dma(shape)]

    return pl.pallas_call(
        functools.partial(stack_kernel, n, dp, mp),
        out_shape=jax.ShapeDtypeStruct((rows, width), bf),
        in_specs=[vmem, vmem, vmem, vmem, vmem, hbm, hbm, hbm],
        out_specs=vmem,
        scratch_shapes=[
            pltpu.VMEM((units, full), bf),
            pltpu.VMEM((units, full), bf),
            pltpu.VMEM((units, full), bf),
            pltpu.VMEM((HALVES, mp, size, width + LANES), bf),
            pltpu.VMEM((HALVES, mp, size, width), bf),
            pltpu.VMEM((HALVES, cores, mp, n * hr, width), bf),
            pltpu.VMEM((HALVES, sides, n * hr, width), bf),
            pltpu.VMEM((HALVES, n, hr, width), bf),
            pltpu.VMEM((HALVES, n, hr, width), bf),
            pltpu.VMEM((HALVES, hr, width), bf),
            pltpu.VMEM((size, units), bf),
            pltpu.VMEM((LAYERS, HALVES, size, 1), f32),
            pltpu.VMEM((2, size, 1), f32),
            pltpu.VMEM(share_shape, f32),
            dma((3,)), *pair(1),
            dma((HALVES,)), dma((HALVES, hops, PARTS)), dma((HALVES,)), dma((HALVES, hops, PARTS)),
            dma((HALVES, sides)), dma((HALVES, n, sides)), *pair(HALVES, cores),
            *pair(HALVES, mp, cores), dma((HALVES, sides)), dma((HALVES, n, PARTS, sides)),
            dma((HALVES,)), dma((HALVES, hops, PARTS)), dma((HALVES,)), dma((HALVES, hops, PARTS)),
            dma((HALVES,)), dma((HALVES, PARTS)),
        ],
        compiler_params=pltpu.CompilerParams(
            collective_id=0, has_side_effects=True, vmem_limit_bytes=67043328
        ),
    )(current, gain, ids, counts, exits, w_gate, w_up, w_down)


def body(hidden_in, norm_gain, expert_ids, gate_counts, exit_layer, w_gate, w_up, w_down):
    n, dp, mp = lax.axis_size("expert"), lax.axis_size("dp"), lax.axis_size("mp")
    return stack(
        n, dp, mp, hidden_in, norm_gain, expert_ids.transpose(0, 2, 1),
        gate_counts.transpose(0, 2, 1), exit_layer[None, :], w_gate, w_up, w_down,
    )


def solution(mesh):
    in_specs = (
        P(("groups", "expert", "dp"), "mp"),
        P(None, "mp"),
        P(None, ("groups", "expert", "dp"), None),
        P(None, ("groups", "expert", "dp"), None),
        P(("groups", "expert", "dp")),
        P(None, "expert", ("mp", "dp"), None),
        P(None, "expert", ("mp", "dp"), None),
        P(None, "expert", ("mp", "dp"), None),
    )
    out_specs = P(("groups", "expert", "dp"), "mp")
    return jax.shard_map(body, mesh=mesh, in_specs=in_specs, out_specs=out_specs, check_vma=False)
```
